16 devices in a mesh: nodes: 16 (over z, y, x, core).
Axes of the slice: x: 2, y: 2, z: 2, core: 2. Of those that a mesh axis runs over, the one named last changes fastest.
Arguments:
- adjacency: bfloat16 [16384, 16384], P('nodes')
- features: bfloat16 [16384, 602], P('nodes')
- w_one: float32 [602, 256], replicated
- w_two: float32 [256, 41], replicated
- labels: int32 [16384], P('nodes')
- label_mask: int32 [16384], P('nodes')
Outputs:
- output 1: float32 [], replicated
- output 2: float32 [602, 256], replicated
- output 3: float32 [256, 41], replicated
All inputs are finite; a program needn't handle non-finite values.
Results may differ from the reference program's by a relative error of at most 0.00194.
Values are sent between devices in bfloat16 or wider.
A program may use at most 1 GiB of HBM per device.

```python
import jax
import jax.numpy as jnp
from jax import lax

NUM_NODES = 16384
F_IN = 602
HIDDEN = 256
CLASSES = 41
COMMUNITIES = 8
EDGE_IN = 40
EDGE_OUT = 8
HASH_MOD = 128
HASH_SHIFT = 2048
HASH_RANGE = 32768
LABEL_RATE = 4


def draw_graph(key_base):
    key_mult, key_add, key_comm = jax.random.split(key_base, 3)
    mult_ids = jax.random.randint(key_mult, (NUM_NODES,), 0, HASH_RANGE, dtype=jnp.int32)
    add_ids = jax.random.randint(key_add, (NUM_NODES,), 0, HASH_RANGE, dtype=jnp.int32)
    comm_ids = jax.random.randint(key_comm, (NUM_NODES,), 0, COMMUNITIES, dtype=jnp.int32)
    hashed = (mult_ids[:, None] * mult_ids[None, :] // HASH_SHIFT + add_ids[:, None] + add_ids[None, :]) % HASH_MOD
    edge_limit = jnp.where(comm_ids[:, None] == comm_ids[None, :], EDGE_IN, EDGE_OUT)
    node_ids = jnp.arange(NUM_NODES, dtype=jnp.int32)
    linked = (hashed < edge_limit) | (node_ids[:, None] == node_ids[None, :])
    degree = jnp.sum(linked.astype(jnp.int32), axis=1).astype(jnp.float32)
    inv_root = lax.rsqrt(degree)
    adjacency = jnp.where(linked, inv_root[:, None] * inv_root[None, :], 0.0).astype(jnp.bfloat16)
    return adjacency, jnp.sqrt(jnp.mean(degree))


def draw_mask(key_base):
    key_rate, key_pick = jax.random.split(key_base)
    chosen = jax.random.randint(key_rate, (NUM_NODES,), 0, LABEL_RATE, dtype=jnp.int32) == 0
    forced = jax.random.randint(key_pick, (), 0, NUM_NODES, dtype=jnp.int32)
    return (chosen | (jnp.arange(NUM_NODES, dtype=jnp.int32) == forced)).astype(jnp.int32)


def setup_inputs(seed: int = 0) -> dict:
    key_base = jax.random.key(seed)
    key_graph, key_feat, key_one, key_two, key_label, key_mask = jax.random.split(key_base, 6)
    adjacency, weight_gain = draw_graph(key_graph)
    features = jax.random.normal(key_feat, (NUM_NODES, F_IN), jnp.float32).astype(jnp.bfloat16)
    w_one = jax.random.normal(key_one, (F_IN, HIDDEN), jnp.float32) * (weight_gain * F_IN ** -0.5)
    raw_two = jax.random.normal(key_two, (HIDDEN, CLASSES), jnp.float32)
    w_two = (raw_two - jnp.mean(raw_two, axis=0, keepdims=True)) * (1.5 * weight_gain * HIDDEN ** -0.5)
    labels = jax.random.randint(key_label, (NUM_NODES,), 0, CLASSES, dtype=jnp.int32)
    label_mask = draw_mask(key_mask)
    return {'adjacency': adjacency, 'features': features, 'w_one': w_one, 'w_two': w_two, 'labels': labels, 'label_mask': label_mask}


def contract_rows(left, right):
    return lax.dot_general(left, right, (((0,), (0,)), ((), ())), preferred_element_type=jnp.float32)


def reference(adjacency, features, w_one, w_two, labels, label_mask):
    w_one_b = w_one.astype(jnp.bfloat16)
    w_two_b = w_two.astype(jnp.bfloat16)
    y_one = jnp.dot(features, w_one_b, preferred_element_type=jnp.float32).astype(jnp.bfloat16)
    z_one = jnp.dot(adjacency, y_one, preferred_element_type=jnp.float32)
    h_one = jnp.maximum(z_one, 0.0).astype(jnp.bfloat16)
    y_two = jnp.dot(h_one, w_two_b, preferred_element_type=jnp.float32).astype(jnp.bfloat16)
    z_two = jnp.dot(adjacency, y_two, preferred_element_type=jnp.float32)
    mask_f = label_mask.astype(jnp.float32)
    label_count = jnp.sum(mask_f)
    log_norm = jax.nn.logsumexp(z_two, axis=1)
    onehot = (labels[:, None] == jnp.arange(CLASSES, dtype=jnp.int32)[None, :]).astype(jnp.float32)
    picked = jnp.sum(z_two * onehot, axis=1)
    loss_value = jnp.sum(mask_f * (log_norm - picked)) / label_count
    soft_probs = jnp.exp(z_two - log_norm[:, None])
    g_two = ((soft_probs - onehot) * (mask_f / label_count)[:, None]).astype(jnp.bfloat16)
    grad_y2 = contract_rows(adjacency, g_two).astype(jnp.bfloat16)
    grad_two = contract_rows(h_one, grad_y2)
    grad_h1 = lax.dot_general(grad_y2, w_two_b, (((1,), (1,)), ((), ())), preferred_element_type=jnp.float32)
    grad_z1 = jnp.where(z_one > 0.0, grad_h1, 0.0).astype(jnp.bfloat16)
    grad_y1 = contract_rows(adjacency, grad_z1).astype(jnp.bfloat16)
    grad_one = contract_rows(features, grad_y1)
    return (loss_value, grad_one, grad_two)
```

```python
import functools

import jax
import jax.numpy as jnp
from jax import lax
from jax.experimental import pallas as pl
from jax.experimental.pallas import tpu as pltpu
from jax.sharding import PartitionSpec as P

MESH = pl.DeviceIdType.MESH
F32 = jnp.float32
BF16 = jnp.bfloat16

N_DEV = 16
ROWS = 1024
HID = 256
CLS_PAD = 48
LANES = 128
FEAT_PAD = 640
CHUNK = FEAT_PAD // N_DEV
SMALL = CLS_PAD + 8

WIDE_PARTS = ((0, 336), (336, 336), (672, 352))
THIN_PARTS = ((0, 16), (16, 16), (32, 16))


def nt(left, right):
    return lax.dot_general(left, right, (((1,), (1,)), ((), ())), preferred_element_type=F32)


def tn(left, right):
    return lax.dot_general(left, right, (((0,), (0,)), ((), ())), preferred_element_type=F32)


def nn(left, right):
    return lax.dot_general(left, right, (((1,), (0,)), ((), ())), preferred_element_type=F32)


def kernel(
    axis,
    classes,
    adj,
    feat,
    w_one,
    w_two,
    labels,
    mask,
    loss_out,
    one_out,
    two_out,
    adj_v,
    y_all,
    d_all,
    y2_all,
    g2_all,
    z_one,
    h_one,
    thin,
    wide,
    w2_pad,
    w2t,
    count,
    count_in,
    small,
    small_in,
    dw,
    dw_in,
    red,
    rs_in,
    fin,
    adj_sem,
    ici_send,
    ici_recv,
    d2d_send,
    d2d_recv,
    ar_send,
    ar_recv,
    fin_send,
    fin_recv,
):
    me = lax.axis_index(axis)
    core = lax.rem(me, 2)
    chip = lax.div(me, 2)
    turn = [(1 - 2 * lax.rem(lax.div(me, 2 << k), 2)) * (2 << k) for k in range(3)]
    partner = me + 1 - 2 * core

    def at(m):
        d = me
        for k in range(3):
            if m >> k & 1:
                d = d + turn[k]
        return d

    def at_other(m):
        return at(m) + 1 - 2 * core

    def chip_at(m):
        return lax.div(at(m), 2)

    sent = []

    def push(src, dst, send_sem, recv_sem, device):
        copy = pltpu.make_async_remote_copy(
            src_ref=src, dst_ref=dst, send_sem=send_sem, recv_sem=recv_sem, device_id=(device,), device_id_type=MESH
        )
        copy.start()
        sent.append(copy)

    def await_recv(dst, send_sem, recv_sem):
        pltpu.make_async_remote_copy(
            src_ref=dst, dst_ref=dst, send_sem=send_sem, recv_sem=recv_sem, device_id=(partner,), device_id_type=MESH
        ).wait_recv()

    class Gather:
        def __init__(self, g, buf, parts):
            self.g, self.buf, self.parts = g, buf, parts

        def piece(self, block, p):
            r0, n = self.parts[p]
            return self.buf.at[block, pl.ds(r0, n)]

        def send(self, m, p, k):
            src = self.piece(at(m), p)
            t = (m ^ (1 << k)) * 3 + p
            push(src, src, ici_send.at[self.g, t], ici_recv.at[self.g, t], at(1 << k))

        def share(self, m, p):
            src = self.piece(at(m), p)
            t = m * 3 + p
            push(src, src, d2d_send.at[self.g, t], d2d_recv.at[self.g, t], partner)

        def got(self, m, p):
            t = m * 3 + p
            await_recv(self.piece(at(m), p), ici_send.at[self.g, t], ici_recv.at[self.g, t])

        def got_other(self, m, p):
            t = m * 3 + p
            await_recv(self.piece(at_other(m), p), d2d_send.at[self.g, t], d2d_recv.at[self.g, t])

        def begin(self):
            for step in range(3):
                for q in range(3):
                    self.send(0, (q - step) % 3, q)
                if step == 0:
                    for p in range(3):
                        self.share(0, p)

        def event(self, e):
            for q in range(3):
                a, b = (q + 1) % 3, (q + 2) % 3
                bit = 1 << q
                if e == 0:
                    m, p, on = bit, q, (a, b)
                elif e == 1:
                    m, p, on = bit, (q - 1) % 3, (a,)
                elif e == 2:
                    m, p, on = bit, (q - 2) % 3, ()
                elif e == 3:
                    m, p, on = bit | 1 << (q - 1) % 3, (q - 1) % 3, (a,)
                elif e == 4:
                    m, p, on = bit | 1 << (q - 2) % 3, (q - 2) % 3, ()
                elif e == 5:
                    m, p, on = bit | 1 << (q - 1) % 3, (q - 2) % 3, ()
                else:
                    m, p, on = 7, (q - 2) % 3, ()
                self.got(m, p)
                for k in on:
                    self.send(m, p, k)
                self.share(m, p)

        def others(self, ms):
            for m in ms:
                for p in range(3):
                    self.got_other(m, p)

    gathers = [
        Gather(0, y_all, WIDE_PARTS),
        Gather(1, y2_all, THIN_PARTS),
        Gather(2, g2_all, THIN_PARTS),
        Gather(3, d_all, WIDE_PARTS),
    ]

    def reduce_send(stage, buf, buf_in, row):
        peer = partner if stage == 0 else at(1 << (stage - 1))
        push(buf.at[stage], buf_in.at[stage], ar_send.at[row, stage], ar_recv.at[row, stage], peer)

    def reduce_add(stage, buf, buf_in, row):
        await_recv(buf_in.at[stage], ar_send.at[row, stage], ar_recv.at[row, stage])
        buf[stage + 1] = buf[stage] + buf_in[stage]

    def adj_copy(block):
        cols = pl.ds(pl.multiple_of(block * ROWS, ROWS), ROWS)
        return pltpu.make_async_copy(adj.at[:, cols], adj_v.at[block], adj_sem.at[block])

    for m in (0, 1, 2, 4, 3, 6, 5, 7):
        adj_copy(at(m)).start()
        adj_copy(at_other(m)).start()

    barrier = pltpu.get_barrier_semaphore()
    greet = [partner] + [at(m) for m in range(1, 8)]
    for peer in greet:
        pl.semaphore_signal(barrier, inc=1, device_id=(peer,), device_id_type=MESH)

    w1b = w_one[...].astype(BF16)
    y_all[me] = nn(feat[...], w1b).astype(BF16)
    count[0] = jnp.full(count.shape[1:], jnp.sum(mask[...].astype(F32)), F32)

    pl.semaphore_wait(barrier, len(greet))

    def passes(gather, first, multiply, hooks):
        multiply(at(0), True)
        hooks(0)

        def run(masks, e):
            devices = [at(m) for m in masks] + [at_other(m) for m in masks]
            n = len(masks)

            def body(i, c):
                if n == 1:
                    block = devices[0] + i * (devices[1] - devices[0])
                else:
                    j, s = lax.rem(i, 3), lax.div(i, 3)
                    three = [d + s * (o - d) for d, o in zip(devices[:3], devices[3:])]
                    block = (
                        three[0] * lax.div((1 - j) * (2 - j), 2)
                        + three[1] * j * (2 - j)
                        + three[2] * lax.div(j * (j - 1), 2)
                    )

                @pl.when(i == n)
                def _():
                    gather.others(masks)

                multiply(block, False)
                return c

            lax.fori_loop(0, 2 * n, body, 0)

        gather.others((0,))
        multiply(at_other(0), False)
        gather.event(0)
        hooks(1)
        gather.event(1)
        gather.event(2)
        hooks(2)
        if first:
            run((1, 2, 4), 0)
            gather.event(3)
            hooks(3)
            gather.event(4)
            gather.event(5)
        else:
            gather.event(3)
            hooks(3)
            run((1, 2, 4), 0)
            gather.event(4)
            gather.event(5)
        hooks(4)
        if not first:
            gather.event(6)
        run((3, 6, 5), 0)
        if first:
            gather.event(6)
        run((7,), 0)

    gathers[0].begin()
    reduce_send(0, count, count_in, 0)

    w2_pad[...] = jnp.zeros_like(w2_pad)
    w2_pad[:, 0:classes] = w_two[...]
    w2t[...] = w2_pad[...].T[0:CLS_PAD].astype(BF16)

    def wide_multiply(src, wait_adj):
        def multiply(block, new):
            if wait_adj:
                adj_copy(block).wait()
            part = nn(adj_v[block], src[block])
            if new:
                wide[...] = part
            else:
                wide[...] += part

        return multiply

    def count_hooks(e):
        if e < 4:
            reduce_add(e, count, count_in, 0)
            if e < 3:
                reduce_send(e + 1, count, count_in, 0)

    passes(gathers[0], True, wide_multiply(y_all, True), count_hooks)
    z_one[...] = wide[...]
    h_one[...] = jnp.maximum(wide[...], 0.0).astype(BF16)

    y2_all[me] = nt(w2t[...], h_one[...]).astype(BF16)
    gathers[1].begin()

    def thin_multiply(src):
        def multiply(block, new):
            part = nt(adj_v[block], src[block])
            if new:
                thin[:, 0:CLS_PAD] = part
            else:
                thin[:, 0:CLS_PAD] += part

        return multiply

    def no_hooks(e):
        pass

    thin[...] = jnp.zeros_like(thin)
    passes(gathers[1], False, thin_multiply(y2_all), no_hooks)

    z2t = thin[...].T[0:CLS_PAD]
    cls = lax.broadcasted_iota(jnp.int32, (CLS_PAD, ROWS), 0)
    real = cls < classes
    top = jnp.max(jnp.where(real, z2t, -jnp.inf), axis=0, keepdims=True)
    total = jnp.sum(jnp.where(real, jnp.exp(z2t - top), 0.0), axis=0, keepdims=True)
    log_norm = top + jnp.log(total)
    onehot = cls == labels[...]
    mask_f = mask[...].astype(F32)
    picked = jnp.sum(jnp.where(onehot, z2t, 0.0), axis=0, keepdims=True)
    loss_part = jnp.sum(mask_f * (log_norm - picked))
    nodes = count[4][0:1, 0:1]
    soft = jnp.exp(z2t - log_norm)
    g2 = (soft - onehot.astype(F32)) * (mask_f / nodes)
    g2_all[me] = jnp.where(real, g2, 0.0).astype(BF16)

    gathers[2].begin()
    passes(gathers[2], False, thin_multiply(g2_all), no_hooks)
    e2 = thin[...].astype(BF16)[:, 0:CLS_PAD]
    grad_h1 = nn(e2, w2t[...])
    d_all[me] = jnp.where(z_one[...] > 0.0, grad_h1, 0.0).astype(BF16)

    gathers[3].begin()
    small[0, 0:CLS_PAD] = tn(e2, h_one[...])
    small[0, CLS_PAD:SMALL] = jnp.full((SMALL - CLS_PAD, HID), loss_part, F32)
    reduce_send(0, small, small_in, 1)

    def small_hooks(e):
        if e < 4:
            reduce_add(e, small, small_in, 1)
            if e < 3:
                reduce_send(e + 1, small, small_in, 1)

    passes(gathers[3], True, wide_multiply(d_all, False), small_hooks)

    half = FEAT_PAD // 2
    features = feat.shape[1]
    dw[FEAT_PAD - LANES :] = jnp.zeros((LANES, HID), F32)
    dw[0:features] = tn(feat[...], wide[...].astype(BF16))
    theirs = pl.multiple_of((1 - core) * half, half)
    mine = pl.multiple_of(core * half, half)
    push(dw.at[pl.ds(theirs, half)], dw_in, fin_send.at[0], fin_recv.at[0], partner)
    await_recv(dw_in, fin_send.at[0], fin_recv.at[0])
    red[...] = (dw[pl.ds(mine, half)] + dw_in[...]).reshape(N_DEV // 2, CHUNK, HID)
    far_first = (7, 3, 6, 5, 1, 2, 4)
    for m in far_first:
        push(red.at[chip_at(m)], rs_in.at[m], fin_send.at[m], fin_recv.at[m], at(m))
    total_dw = red[chip]
    for m in (1, 2, 4, 3, 6, 5, 7):
        await_recv(rs_in.at[m], fin_send.at[m], fin_recv.at[m])
        total_dw = total_dw + rs_in[m]
    own = core * 8 + chip
    fin[own] = total_dw
    for m in far_first:
        push(fin.at[own], fin.at[own], fin_send.at[8 + m], fin_recv.at[8 + m], at(m))
    push(fin.at[own], fin.at[own], fin_send.at[16], fin_recv.at[16], partner)
    for m in (1, 2, 4, 3, 6, 5, 7):
        there = core * 8 + chip_at(m)
        await_recv(fin.at[there], fin_send.at[8 + m], fin_recv.at[8 + m])
        push(fin.at[there], fin.at[there], fin_send.at[16 + m], fin_recv.at[16 + m], partner)

    two_out[:, 0:CLS_PAD] = small[4][0:CLS_PAD].T
    loss_out[...] = small[4][CLS_PAD:SMALL, 0:LANES] / count[4]

    for m in (0, 1, 2, 4, 3, 6, 5, 7):
        there = (1 - core) * 8 + chip_at(m)
        await_recv(fin.at[there], fin_send.at[16 + m], fin_recv.at[16 + m])
    one_out[...] = fin[...]
    for copy in sent:
        copy.wait_send()


def solution(mesh):
    axis = mesh.axis_names[0]

    def local_step(adj_rows, feat_rows, w_one, w_two, label_rows, mask_rows):
        classes = w_two.shape[1]
        vmem = pl.BlockSpec(memory_space=pltpu.VMEM)
        loss, one, two = pl.pallas_call(
            functools.partial(kernel, axis, classes),
            out_shape=(
                jax.ShapeDtypeStruct((8, LANES), F32),
                jax.ShapeDtypeStruct((N_DEV, CHUNK, HID), F32),
                jax.ShapeDtypeStruct((HID, LANES), F32),
            ),
            in_specs=[pl.BlockSpec(memory_space=pl.ANY)] + [vmem] * 5,
            out_specs=(vmem, vmem, vmem),
            scratch_shapes=[
                pltpu.VMEM((N_DEV, ROWS, ROWS), BF16),
                pltpu.VMEM((N_DEV, ROWS, HID), BF16),
                pltpu.VMEM((N_DEV, ROWS, HID), BF16),
                pltpu.VMEM((N_DEV, CLS_PAD, ROWS), BF16),
                pltpu.VMEM((N_DEV, CLS_PAD, ROWS), BF16),
                pltpu.VMEM((ROWS, HID), F32),
                pltpu.VMEM((ROWS, HID), BF16),
                pltpu.VMEM((ROWS, LANES), F32),
                pltpu.VMEM((ROWS, HID), F32),
                pltpu.VMEM((HID, LANES), F32),
                pltpu.VMEM((CLS_PAD, HID), BF16),
                pltpu.VMEM((5, 8, LANES), F32),
                pltpu.VMEM((4, 8, LANES), F32),
                pltpu.VMEM((5, SMALL, HID), F32),
                pltpu.VMEM((4, SMALL, HID), F32),
                pltpu.VMEM((FEAT_PAD, HID), F32),
                pltpu.VMEM((FEAT_PAD // 2, HID), F32),
                pltpu.VMEM((N_DEV // 2, CHUNK, HID), F32),
                pltpu.VMEM((N_DEV // 2, CHUNK, HID), F32),
                pltpu.VMEM((N_DEV, CHUNK, HID), F32),
                pltpu.SemaphoreType.DMA((N_DEV,)),
                pltpu.SemaphoreType.DMA((4, 24)),
                pltpu.SemaphoreType.DMA((4, 24)),
                pltpu.SemaphoreType.DMA((4, 24)),
                pltpu.SemaphoreType.DMA((4, 24)),
                pltpu.SemaphoreType.DMA((2, 4)),
                pltpu.SemaphoreType.DMA((2, 4)),
                pltpu.SemaphoreType.DMA((24,)),
                pltpu.SemaphoreType.DMA((24,)),
            ],
            compiler_params=pltpu.CompilerParams(
                collective_id=0, has_side_effects=True, vmem_limit_bytes=67_043_328
            ),
            name="gcn_step",
        )(adj_rows, feat_rows, w_one, w_two, label_rows.reshape(1, -1), mask_rows.reshape(1, -1))
        one = one.reshape(FEAT_PAD, HID)[: w_one.shape[0]]
        return loss[0, 0], one, two[:, :classes]

    return jax.shard_map(
        local_step,
        mesh=mesh,
        in_specs=(P(axis, None), P(axis, None), P(None, None), P(None, None), P(axis), P(axis)),
        out_specs=(P(), P(None, None), P(None, None)),
        check_vma=False,
    )
```
